32 devices in a mesh: section: 4 (over z), dp: 8 (over y, x, core).
Axes of the slice: x: 2, y: 2, z: 4, core: 2. Of those that a mesh axis runs over, the one named last changes fastest.
Arguments:
- entry: bfloat16 [1536, 3584], P('dp'), may hold values from -6 to 6
- norm_gain: float32 [4, 3584], P('section'), may hold values from 0.5 to 1.5
- w_qkv: bfloat16 [4, 3584, 1152], P('section', 'dp'), may hold values from -0.09375 to 0.09375
- w_out: bfloat16 [4, 896, 3584], P('section', 'dp'), may hold values from -0.1875 to 0.1875
- final_gain: float32 [3584], replicated, may hold values from 0.5 to 1.5
- lengths: int32 [32], P('dp'), may hold values from 24 to 48
- positive: int32 [16], P('dp'), may hold values from 0 to 15, each once
Outputs:
- section_grads: bfloat16 [4, 1536, 3584], P('section', 'dp')
The draws below stay inside these ranges and needn't reach their ends.
Inputs may be any that keep to these rules, and one draw needn't show every extreme that they name: lengths[j] is the count of tokens of sequence j; its last token is pooled. Each document index is the positive of exactly one query.
All inputs are finite; a program needn't handle non-finite values.
Results may differ from the reference program's by a relative error of at most 0.022.
Values may be sent and summed in bfloat16 or wider, within the bound.
A program may use at most 192 MiB of HBM per device.

```python
import jax
import jax.numpy as jnp
from jax import lax

D = 3584
HEAD_DIM = 64
GROUP_HEADS = 7
KV_GROUPS = 2
LEN = 48
QW = 896
QUERIES = 16
SEQS = 32
TOKENS = 1536
N_SECTION = 4


def place_ends(values, rng, smallest, high):
    index_at = [jax.random.randint(jax.random.fold_in(rng, axis), (), 0, length) for axis, length in enumerate(values.shape)]
    main_axis = values.shape.index(max(values.shape))
    next_to = index_at[:main_axis] + [(index_at[main_axis] + 1) % values.shape[main_axis]] + index_at[main_axis + 1:]
    return values.at[tuple(index_at)].set(smallest).at[tuple(next_to)].set(high)


def shard_levels(rng, dims, shards, smallest, high):
    def one(axis_at, shards_of):
        steps = jax.random.uniform(jax.random.fold_in(jax.random.fold_in(rng, 6), axis_at), (shards_of,), jnp.float32, smallest / len(shards), high / len(shards))
        return jnp.repeat(jnp.exp(steps), dims[axis_at] // shards_of).reshape((-1,) + (1,) * (len(dims) - axis_at - 1))

    level = one(*shards[0])
    for cut in shards[1:]:
        level = level * one(*cut)
    return level


def noise(rng, dims, deviation, reach, shards=(), kind=jnp.bfloat16):
    drawn = jax.random.normal(rng, dims, jnp.float32) * deviation
    if len(shards) > 0:
        drawn = shard_levels(rng, dims, shards, -0.22, 0.18) * drawn
    return jnp.clip(drawn, min=-reach, max=reach).astype(kind)


def setup_inputs(seed: int = 0) -> dict:
    arg_keys = jax.random.split(jax.random.key(seed), 8)
    return {
        "entry": noise(arg_keys[0], (TOKENS, D), 1.0, 6.0, ((0, 8),)),
        "norm_gain": jnp.clip(1.0 + 0.1 * jax.random.normal(arg_keys[1], (N_SECTION, D), jnp.float32), 0.5, 1.5),
        "w_qkv": noise(arg_keys[2], (N_SECTION, D, QW + 2 * KV_GROUPS * HEAD_DIM), D ** -0.5, 0.09375, ((0, 4), (1, 8))),
        "w_out": noise(arg_keys[3], (N_SECTION, QW, D), QW ** -0.5, 0.1875, ((0, 4), (1, 8))),
        "final_gain": jnp.clip(1.0 + 0.1 * jax.random.normal(arg_keys[4], (D,), jnp.float32), 0.5, 1.5),
        "lengths": place_ends(jax.random.randint(arg_keys[5], (SEQS,), LEN // 2, LEN + 1), jax.random.fold_in(arg_keys[5], 1), LEN // 2, LEN).astype(jnp.int32),
        "positive": jax.random.permutation(arg_keys[6], QUERIES).astype(jnp.int32),
    }


rope_base = 1000000.0
norm_eps = 1e-06
sharpness_divisor = 0.05
objective_coefficient = 256.0

def rotary(values, positions):
    half_dim = values.shape[-1] // 2
    frequency = rope_base ** (-jnp.arange(half_dim, dtype=jnp.float32) * (2.0 / values.shape[-1]))
    angles = positions.astype(jnp.float32)[:, None] * frequency[None, :]
    cosine = jnp.cos(angles)[:, None, :]
    sine_part = jnp.sin(angles)[:, None, :]
    first_half = values[..., :half_dim]
    second_half = values[..., half_dim:]
    return jnp.concatenate([first_half * cosine - second_half * sine_part, second_half * cosine + first_half * sine_part], axis=-1)

def rms_scale(values, gain_row):
    return values * lax.rsqrt(lax.optimization_barrier(jnp.mean(values * values, axis=-1, keepdims=True)) + norm_eps) * gain_row

def attention_layer(hidden, seq_lengths, gain_row, weight_qkv, weight_out):
    row_count, row_width = hidden.shape
    seq_count = seq_lengths.shape[0]
    length = row_count // seq_count
    q_width = weight_out.shape[0]
    kv_width = KV_GROUPS * HEAD_DIM
    wide_in = hidden.astype(jnp.float32)
    normed = rms_scale(wide_in, gain_row).astype(jnp.bfloat16)
    projected = jnp.dot(normed, weight_qkv, preferred_element_type=jnp.float32)
    positions = jnp.arange(length, dtype=jnp.int32)
    query_rot = rotary(projected[:, :q_width].reshape(seq_count, length, KV_GROUPS * GROUP_HEADS, HEAD_DIM), positions).astype(jnp.bfloat16)
    key_rot = rotary(projected[:, q_width:q_width + kv_width].reshape(seq_count, length, KV_GROUPS, HEAD_DIM), positions).astype(jnp.bfloat16)
    value_rows = projected[:, q_width + kv_width:].reshape(seq_count, length, KV_GROUPS, HEAD_DIM).astype(jnp.bfloat16)
    query_grid = query_rot.reshape(seq_count, length, KV_GROUPS, GROUP_HEADS, HEAD_DIM)
    scores = jnp.einsum('sqgzd,skgd->sgzqk', query_grid.astype(jnp.float32), key_rot.astype(jnp.float32)) * HEAD_DIM ** (-0.5)
    key_live = positions[None, :] < seq_lengths[:, None]
    weights = jnp.where(key_live[:, None, None, None, :], jnp.exp(scores), 0.0)
    prob_low = (weights / lax.optimization_barrier(jnp.sum(weights, axis=-1, keepdims=True))).astype(jnp.bfloat16)
    context = jnp.einsum('sgzqk,skgd->sqgzd', prob_low.astype(jnp.float32), value_rows.astype(jnp.float32)).astype(jnp.bfloat16)
    branch = jnp.dot(context.reshape(row_count, q_width), weight_out, preferred_element_type=jnp.float32)
    return (wide_in + branch).astype(jnp.bfloat16)

def embed_rows(rows_in, final_gain):
    pooled = rms_scale(rows_in.astype(jnp.float32), final_gain)
    return pooled * lax.rsqrt(lax.optimization_barrier(jnp.sum(pooled * pooled, axis=-1, keepdims=True)))

def pair_terms(question_representation, passage_representation, positive):
    match_raw_scores = jnp.dot(question_representation, passage_representation.T, preferred_element_type=jnp.float32) * (1.0 / sharpness_divisor)
    weights = jnp.exp(match_raw_scores)
    normalized_exponential_odds = weights / lax.optimization_barrier(jnp.sum(weights, axis=-1, keepdims=True))
    correct_target_column = (positive[:, None] == jnp.arange(passage_representation.shape[0], dtype=jnp.int32)[None, :]).astype(jnp.float32)
    return (normalized_exponential_odds - correct_target_column) * (objective_coefficient / sharpness_divisor)

def reference(entry, norm_gain, w_qkv, w_out, final_gain, lengths, positive):
    section_count = norm_gain.shape[0]
    seq_count = lengths.shape[0]
    length = entry.shape[0] // seq_count
    row_width = entry.shape[1]
    hidden = entry
    inputs = []
    for layer_id in range(section_count):
        inputs.append(hidden)
        hidden = attention_layer(hidden, lengths, norm_gain[layer_id], w_qkv[layer_id], w_out[layer_id])
    seq_grid = hidden.reshape(seq_count, length, row_width)
    last_rows = jnp.take_along_axis(seq_grid, (lengths - 1)[:, None, None], axis=1)[:, 0]
    embedding, back_embed = jax.vjp(lambda rows_in: embed_rows(rows_in, final_gain), last_rows)
    emb_low = embedding.astype(jnp.bfloat16)
    question_representation = emb_low[0::2]
    passage_representation = emb_low[1::2]
    pair_coef = pair_terms(question_representation, passage_representation, positive)
    grad_query = jnp.dot(pair_coef, passage_representation.astype(jnp.float32), precision=lax.Precision.HIGHEST)
    grad_doc = jnp.dot(pair_coef.T, question_representation.astype(jnp.float32), precision=lax.Precision.HIGHEST)
    grad_emb = jnp.stack([grad_query, grad_doc], axis=1).reshape(seq_count, row_width)
    grad_last = back_embed(grad_emb)[0]
    slot_hit = jnp.arange(length, dtype=jnp.int32)[None, :] == (lengths - 1)[:, None]
    seed_grad = jnp.where(slot_hit[:, :, None], grad_last[:, None, :], 0).astype(jnp.bfloat16).reshape(-1, row_width)
    cotangent = seed_grad
    collected = []
    for layer_id in reversed(range(section_count)):
        _, pull_back = jax.vjp(lambda values: attention_layer(values, lengths, norm_gain[layer_id], w_qkv[layer_id], w_out[layer_id]), inputs[layer_id])
        cotangent = pull_back(cotangent)[0]
        collected.append(cotangent)
    return jnp.stack(collected[::-1])
```

```python
import functools

import jax
import jax.numpy as jnp
import numpy as np
from jax import lax
from jax.experimental import pallas as pl
from jax.experimental.pallas import tpu as pltpu
from jax.sharding import PartitionSpec as P

HEAD_DIM = 64
GROUP_HEADS = 7
KV_GROUPS = 2
HEADS = GROUP_HEADS * KV_GROUPS
ROPE_BASE = 1000000.0
EPS = 1e-06
SHARPNESS = 20.0
COEF = 256.0
MESH = pl.DeviceIdType.MESH
F32 = jnp.float32
BF16 = jnp.bfloat16
HI = lax.Precision.HIGHEST


def dot_nn(a, b):
    return lax.dot_general(a, b, (((1,), (0,)), ((), ())), preferred_element_type=F32)


def dot_nt(a, b):
    return lax.dot_general(a, b, (((1,), (1,)), ((), ())), preferred_element_type=F32)


def dot_tn(a, b):
    return lax.dot_general(a, b, (((0,), (0,)), ((), ())), preferred_element_type=F32)


def dot_hi(a, b):
    return lax.dot_general(
        a, b, (((1,), (0,)), ((), ())), preferred_element_type=F32, precision=HI
    )


def rotate(x, cos, sin_signed):
    width = x.shape[-1]
    lane = lax.broadcasted_iota(jnp.int32, x.shape, 1)
    first = lax.rem(lane, HEAD_DIM) < HEAD_DIM // 2
    ahead = pltpu.roll(x, width - HEAD_DIM // 2, 1)
    behind = pltpu.roll(x, HEAD_DIM // 2, 1)
    return x * cos + jnp.where(first, ahead, behind) * sin_signed


def low_half(shape):
    return lax.broadcasted_iota(jnp.int32, shape, 1) < HEAD_DIM


def both_halves(tile):
    wide = tile.astype(F32)
    turned = pltpu.roll(wide, HEAD_DIM, 1)
    low = low_half(wide.shape)
    return (
        jnp.where(low, wide, turned).astype(BF16),
        jnp.where(low, turned, wide).astype(BF16),
    )


def stack_heads(rows, group):
    parts = []
    for head in range(group * GROUP_HEADS, (group + 1) * GROUP_HEADS):
        tile = rows[:, head // 2 * 128 : head // 2 * 128 + 128].astype(F32)
        low = low_half(tile.shape)
        keep = low if head % 2 == 0 else jnp.logical_not(low)
        parts.append(jnp.where(keep, tile, 0.0).astype(BF16))
    return jnp.concatenate(parts, axis=0)


def merge_heads(stacks, length):
    tiles = []
    for pair in range(HEADS // 2):
        halves = []
        for head in (2 * pair, 2 * pair + 1):
            at = head % GROUP_HEADS * length
            halves.append(stacks[head // GROUP_HEADS][at : at + length])
        tiles.append(jnp.where(low_half(halves[0].shape), halves[0], halves[1]))
    return jnp.concatenate(tiles, axis=1)


def fold_groups(sums):
    full = [value + pltpu.roll(value, HEAD_DIM, 1) for value in sums]
    return jnp.where(low_half(full[0].shape), full[0], full[1])


def rms_of(wide):
    return lax.rsqrt(jnp.mean(wide * wide, axis=-1, keepdims=True) + EPS)


def kernel(
    n_sec, n_dp, seqs, length,
    entry, gain, wqkv, wout, final_gain, cos_ref, sin_ref, lengths, positive,
    out,
    hin, hout, gin, xs, probs, rows_buf, emb_all, pos_all,
    f_send, f_recv, b_send, b_recv, e_send, e_recv, p_send, p_recv,
):
    sec = lax.axis_index("section")
    rep = lax.axis_index("dp")
    last = n_sec - 1
    width = entry.shape[-1]
    qw = wout.shape[0]
    blocks = 16 // seqs
    part = width // blocks
    micro = seqs // 2

    barrier = pltpu.get_barrier_semaphore()

    def peer(step):
        return lax.rem(rep + step, n_dp)

    for near in (lax.rem(sec + 1, n_sec), lax.rem(sec + n_sec - 1, n_sec)):
        pl.semaphore_signal(barrier, inc=1, device_id={"section": near}, device_id_type=MESH)
    for step in range(1, n_dp):
        pl.semaphore_signal(barrier, inc=1, device_id={"dp": peer(step)}, device_id_type=MESH)
    pl.semaphore_wait(barrier, n_dp + 1)

    def forward_copy(m):
        return pltpu.make_async_remote_copy(
            src_ref=hout.at[m], dst_ref=hin.at[m], send_sem=f_send.at[m], recv_sem=f_recv.at[m],
            device_id={"section": sec + 1}, device_id_type=MESH,
        )

    def backward_copy(m):
        return pltpu.make_async_remote_copy(
            src_ref=out.at[m], dst_ref=gin.at[m], send_sem=b_send.at[m], recv_sem=b_recv.at[m],
            device_id={"section": sec - 1}, device_id_type=MESH,
        )

    @pl.when(sec == 0)
    def _():
        hin[...] = entry[...]

    def live_keys(m):
        keys = lax.broadcasted_iota(jnp.int32, (GROUP_HEADS * length, length), 1)
        return keys < lengths[m]

    def forward(m, carry):
        @pl.when(sec > 0)
        def _():
            forward_copy(m).wait_recv()

        wide = hin[m].astype(F32)
        normed = (wide * rms_of(wide) * gain[...]).astype(BF16)
        x = rotate(dot_nn(normed, wqkv[...]), cos_ref[...], sin_ref[...]).astype(BF16)
        xs[m] = x
        keys = both_halves(x[:, qw : qw + 128])
        values = both_halves(x[:, qw + 128 : qw + 256])
        live = live_keys(m)
        stacks = []
        for group in range(KV_GROUPS):
            scores = dot_nt(stack_heads(x, group), keys[group]) * HEAD_DIM ** (-0.5)
            weights = jnp.where(live, jnp.exp(scores), 0.0)
            prob = weights / jnp.sum(weights, axis=-1, keepdims=True)
            probs[m, group] = prob
            stacks.append(dot_nn(prob.astype(BF16), values[group]))
        context = merge_heads(stacks, length).astype(BF16)
        hout[m] = (wide + dot_nn(context, wout[...])).astype(BF16)

        @pl.when(sec < last)
        def _():
            forward_copy(m).start()

        return carry

    lax.fori_loop(0, seqs, forward, 0)

    @pl.when(sec == last)
    def _():
        fgain = final_gain[...]
        row16 = lax.broadcasted_iota(jnp.int32, (16, part), 0)
        position = lax.broadcasted_iota(jnp.int32, (length, width), 0)
        own = jnp.zeros((16, part), F32)
        for j in range(seqs):
            picked = jnp.where(position == lengths[j] - 1, hout[j].astype(F32), 0.0)
            row = jnp.sum(picked, axis=0, keepdims=True)
            rows_buf[j] = row
            pooled = row * rms_of(row) * fgain
            unit = pooled * lax.rsqrt(jnp.sum(pooled * pooled, axis=-1, keepdims=True))
            for b in range(blocks):
                own = jnp.where(row16 == b * seqs + j, unit[:, b * part : (b + 1) * part], own)
        emb_all[rep] = own.astype(BF16)
        marks = jnp.zeros((8, 128), jnp.int32)
        mark_row = lax.broadcasted_iota(jnp.int32, (8, 128), 0)
        for i in range(micro):
            marks = jnp.where(mark_row == i, positive[i], marks)
        pos_all[rep] = marks

        def exchange(step):
            to = peer(step)
            return [
                pltpu.make_async_remote_copy(
                    src_ref=buf.at[rep], dst_ref=buf.at[rep],
                    send_sem=send.at[step], recv_sem=recv.at[step],
                    device_id={"dp": to}, device_id_type=MESH,
                )
                for buf, send, recv in ((emb_all, e_send, e_recv), (pos_all, p_send, p_recv))
            ]

        copies = [exchange(step) for step in range(1, n_dp)]
        for pair in copies:
            for copy in pair:
                copy.start()
        for pair in copies:
            for copy in pair:
                copy.wait()

        total = n_dp * seqs
        tall = n_dp * 16
        everyone = emb_all[...].reshape(tall, part)
        cross = dot_nt(everyone, everyone)
        ra = lax.broadcasted_iota(jnp.int32, (tall, tall), 0)
        ca = lax.broadcasted_iota(jnp.int32, (tall, tall), 1)
        same = lax.rem(ra, 16) // seqs == lax.rem(ca, 16) // seqs
        cross = jnp.where(same, cross, 0.0)
        fr = lax.broadcasted_iota(jnp.int32, (total, tall), 0)
        fc = lax.broadcasted_iota(jnp.int32, (total, tall), 1)
        fold = (fc // 16 * seqs + lax.rem(fc, seqs) == fr).astype(F32)
        logits = SHARPNESS * lax.dot_general(
            dot_hi(fold, cross), fold, (((1,), (1,)), ((), ())),
            preferred_element_type=F32, precision=HI,
        )
        qr = lax.broadcasted_iota(jnp.int32, (total, total), 0)
        dc = lax.broadcasted_iota(jnp.int32, (total, total), 1)
        doc = lax.rem(dc, 2) == 1
        weights = jnp.where(doc, jnp.exp(logits), 0.0)
        odds = weights / jnp.sum(weights, axis=-1, keepdims=True)
        marks_all = pos_all[...].reshape(n_dp * 8, 128).astype(F32)
        pr = lax.broadcasted_iota(jnp.int32, (total, n_dp * 8), 0)
        pc = lax.broadcasted_iota(jnp.int32, (total, n_dp * 8), 1)
        pick = (pr // seqs * 8 + lax.rem(pr, seqs) // 2 == pc).astype(F32)
        target = dot_hi(pick, marks_all)[:, :1]
        hit = jnp.logical_and(doc, (dc // 2).astype(F32) == target).astype(F32)
        coef = (odds - hit) * (COEF * SHARPNESS)
        coef = jnp.where(lax.rem(qr, 2) == 0, coef, 0.0)
        both = coef + coef.T
        ar = lax.broadcasted_iota(jnp.int32, (16, total), 0)
        ac = lax.broadcasted_iota(jnp.int32, (16, total), 1)
        mine = (rep * seqs + lax.rem(ar, seqs) == ac).astype(F32)
        spread = dot_hi(dot_hi(mine, both), fold)
        br = lax.broadcasted_iota(jnp.int32, (16, tall), 0)
        bc = lax.broadcasted_iota(jnp.int32, (16, tall), 1)
        spread = jnp.where(br // seqs == lax.rem(bc, 16) // seqs, spread, 0.0)
        grad16 = dot_hi(spread, everyone.astype(F32))
        for j in range(seqs):
            grad_e = jnp.concatenate(
                [grad16[b * seqs + j : b * seqs + j + 1] for b in range(blocks)], axis=1
            )
            row = rows_buf[j]
            scale = rms_of(row)
            pooled = row * scale * fgain
            size = lax.rsqrt(jnp.sum(pooled * pooled, axis=-1, keepdims=True))
            unit = pooled * size
            grad_f = size * (grad_e - unit * jnp.sum(unit * grad_e, axis=-1, keepdims=True))
            grad_n = grad_f * fgain
            grad_r = grad_n * scale - row * (
                scale * scale * scale * jnp.mean(row * grad_n, axis=-1, keepdims=True)
            )
            gin[j] = jnp.where(position == lengths[j] - 1, grad_r, 0.0).astype(BF16)

    def backward(m, carry):
        @pl.when(sec < last)
        def _():
            backward_copy(m).wait_recv()

        grad = gin[m]
        x = xs[m]
        keys = both_halves(x[:, qw : qw + 128])
        values = both_halves(x[:, qw + 128 : qw + 256])
        grad_ctx = dot_nt(grad, wout[...]).astype(BF16)
        grad_q, grad_k, grad_v = [], [], []
        for group in range(KV_GROUPS):
            prob = probs[m, group]
            upper = stack_heads(grad_ctx, group)
            grad_p = dot_nt(upper, values[group]).astype(BF16).astype(F32)
            grad_v.append(dot_tn(prob.astype(BF16), upper))
            inner = jnp.sum(grad_p * prob, axis=-1, keepdims=True)
            grad_s = (prob * (grad_p - inner) * HEAD_DIM ** (-0.5)).astype(BF16)
            grad_q.append(dot_nn(grad_s, keys[group]))
            grad_k.append(dot_tn(grad_s, stack_heads(x, group)))
        grad_x = jnp.concatenate(
            [merge_heads(grad_q, length), fold_groups(grad_k), fold_groups(grad_v)], axis=1
        )
        grad_x = grad_x.astype(BF16).astype(F32)
        grad_x = rotate(grad_x, cos_ref[...], -sin_ref[...]).astype(BF16)
        grad_n = dot_nt(grad_x, wqkv[...]).astype(BF16).astype(F32) * gain[...]
        wide = hin[m].astype(F32)
        scale = rms_of(wide)
        slope = scale * scale * scale * jnp.mean(wide * grad_n, axis=-1, keepdims=True)
        out[m] = (grad.astype(F32) + grad_n * scale - wide * slope).astype(BF16)

        @pl.when(sec > 0)
        def _():
            backward_copy(m).start()

        return carry

    lax.fori_loop(0, seqs, backward, 0)

    @pl.when(sec < last)
    def _():
        for m in range(seqs):
            forward_copy(m).wait_send()

    @pl.when(sec > 0)
    def _():
        for m in range(seqs):
            backward_copy(m).wait_send()


def tables(length, qw, columns):
    lane = np.arange(columns)
    half = HEAD_DIM // 2
    frequency = np.float32(ROPE_BASE) ** (
        -(lane % half).astype(np.float32) * np.float32(2.0 / HEAD_DIM)
    )
    angles = np.arange(length, dtype=np.float32)[:, None] * frequency[None, :]
    turned = (lane < columns - KV_GROUPS * HEAD_DIM)[None, :]
    sign = np.where(lane % HEAD_DIM < half, -1.0, 1.0)[None, :]
    cos = np.where(turned, np.cos(angles), 1.0).astype(np.float32)
    sin = np.where(turned, np.sin(angles) * sign, 0.0).astype(np.float32)
    return jnp.asarray(cos), jnp.asarray(sin)


def per_device(entry, norm_gain, w_qkv, w_out, final_gain, lengths, positive):
    n_sec = lax.axis_size("section")
    n_dp = lax.axis_size("dp")
    seqs = lengths.shape[0]
    rows, width = entry.shape
    length = rows // seqs
    full_qkv = lax.all_gather(w_qkv, "dp", axis=1, tiled=True)[0]
    full_out = lax.all_gather(w_out, "dp", axis=1, tiled=True)[0]
    qw = full_out.shape[0]
    columns = full_qkv.shape[1]
    cos, sin = tables(length, qw, columns)
    vmem = pl.BlockSpec(memory_space=pltpu.VMEM)
    smem = pl.BlockSpec(memory_space=pltpu.SMEM)
    part = width // (16 // seqs)
    dma = pltpu.SemaphoreType.DMA
    block = (seqs, length, width)
    result = pl.pallas_call(
        functools.partial(kernel, n_sec, n_dp, seqs, length),
        out_shape=jax.ShapeDtypeStruct(block, BF16),
        in_specs=[vmem] * 7 + [smem] * 2,
        out_specs=vmem,
        scratch_shapes=[
            pltpu.VMEM(block, BF16),
            pltpu.VMEM(block, BF16),
            pltpu.VMEM(block, BF16),
            pltpu.VMEM((seqs, length, columns), BF16),
            pltpu.VMEM((seqs, KV_GROUPS, GROUP_HEADS * length, length), F32),
            pltpu.VMEM((seqs, 1, width), F32),
            pltpu.VMEM((n_dp, 16, part), BF16),
            pltpu.VMEM((n_dp, 8, 128), jnp.int32),
            dma((seqs,)), dma((seqs,)), dma((seqs,)), dma((seqs,)),
            dma((n_dp,)), dma((n_dp,)), dma((n_dp,)), dma((n_dp,)),
        ],
        compiler_params=pltpu.CompilerParams(
            collective_id=0, has_side_effects=True, vmem_limit_bytes=60 * 1024 * 1024
        ),
    )(
        entry.reshape(block), norm_gain, full_qkv, full_out, final_gain.reshape(1, width),
        cos, sin, lengths, positive,
    )
    return result.reshape(1, rows, width)


def solution(mesh):
    return jax.shard_map(
        per_device,
        mesh=mesh,
        in_specs=(
            P("dp", None),
            P("section", None),
            P("section", "dp", None),
            P("section", "dp", None),
            P(),
            P("dp"),
            P("dp"),
        ),
        out_specs=P("section", "dp", None),
        check_vma=False,
    )
```

```python
import functools

import jax
import jax.numpy as jnp
import numpy as np
from jax import lax
from jax.experimental import pallas as pl
from jax.experimental.pallas import tpu as pltpu
from jax.sharding import PartitionSpec as P

HEAD_DIM = 64
GROUP_HEADS = 7
KV_GROUPS = 2
HEADS = GROUP_HEADS * KV_GROUPS
ROPE_BASE = 1000000.0
EPS = 1e-06
SHARPNESS = 20.0
COEF = 256.0
MESH = pl.DeviceIdType.MESH
F32 = jnp.float32
BF16 = jnp.bfloat16
HI = lax.Precision.HIGHEST


def dot_nn(a, b):
    return lax.dot_general(a, b, (((1,), (0,)), ((), ())), preferred_element_type=F32)


def dot_nt(a, b):
    return lax.dot_general(a, b, (((1,), (1,)), ((), ())), preferred_element_type=F32)


def dot_tn(a, b):
    return lax.dot_general(a, b, (((0,), (0,)), ((), ())), preferred_element_type=F32)


def dot_hi(a, b):
    return lax.dot_general(
        a, b, (((1,), (0,)), ((), ())), preferred_element_type=F32, precision=HI
    )


def rotate(x, cos, sin_signed):
    width = x.shape[-1]
    lane = lax.broadcasted_iota(jnp.int32, x.shape, 1)
    first = lax.rem(lane, HEAD_DIM) < HEAD_DIM // 2
    ahead = pltpu.roll(x, width - HEAD_DIM // 2, 1)
    behind = pltpu.roll(x, HEAD_DIM // 2, 1)
    return x * cos + jnp.where(first, ahead, behind) * sin_signed


def low_half(shape):
    return lax.broadcasted_iota(jnp.int32, shape, 1) < HEAD_DIM


def both_halves(tile):
    wide = tile.astype(F32)
    turned = pltpu.roll(wide, HEAD_DIM, 1)
    low = low_half(wide.shape)
    return (
        jnp.where(low, wide, turned).astype(BF16),
        jnp.where(low, turned, wide).astype(BF16),
    )


def stack_heads(rows, group):
    parts = []
    for head in range(group * GROUP_HEADS, (group + 1) * GROUP_HEADS):
        tile = rows[:, head // 2 * 128 : head // 2 * 128 + 128].astype(F32)
        low = low_half(tile.shape)
        keep = low if head % 2 == 0 else jnp.logical_not(low)
        parts.append(jnp.where(keep, tile, 0.0).astype(BF16))
    return jnp.concatenate(parts, axis=0)


def merge_heads(stacks, length):
    tiles = []
    for pair in range(HEADS // 2):
        halves = []
        for head in (2 * pair, 2 * pair + 1):
            at = head % GROUP_HEADS * length
            halves.append(stacks[head // GROUP_HEADS][at : at + length])
        tiles.append(jnp.where(low_half(halves[0].shape), halves[0], halves[1]))
    return jnp.concatenate(tiles, axis=1)


def fold_groups(sums):
    full = [value + pltpu.roll(value, HEAD_DIM, 1) for value in sums]
    return jnp.where(low_half(full[0].shape), full[0], full[1])


def rms_of(wide):
    return lax.rsqrt(jnp.mean(wide * wide, axis=-1, keepdims=True) + EPS)


def kernel(
    n_sec, n_dp, seqs, length, ring,
    entry, gain, w_in, w_up, final_gain, cos_ref, sin_ref, lengths, positive,
    out,
    hin, hout, gin, xs, probs, rows_buf, emb_all, pos_all, contexts,
    f_send, f_recv, b_send, b_recv, e_send, e_recv, p_send, p_recv,
    *gathering,
):
    sec = lax.axis_index("section")
    rep = lax.axis_index("dp")
    last = n_sec - 1
    width = entry.shape[-1]
    wqkv, wout = gathering[:2] if ring else (w_in, w_up)
    qw = wout.shape[0]
    blocks = 16 // seqs
    part = width // blocks
    micro = seqs // 2

    barrier = pltpu.get_barrier_semaphore()

    def peer(step):
        return lax.rem(rep + step, n_dp)

    for near in (lax.rem(sec + 1, n_sec), lax.rem(sec + n_sec - 1, n_sec)):
        pl.semaphore_signal(barrier, inc=1, device_id={"section": near}, device_id_type=MESH)
    for step in range(1, n_dp):
        pl.semaphore_signal(barrier, inc=1, device_id={"dp": peer(step)}, device_id_type=MESH)
    pl.semaphore_wait(barrier, n_dp + 1)

    def forward_copy(m):
        return pltpu.make_async_remote_copy(
            src_ref=hout.at[m], dst_ref=hin.at[m], send_sem=f_send.at[m], recv_sem=f_recv.at[m],
            device_id={"section": sec + 1}, device_id_type=MESH,
        )

    def backward_copy(m):
        return pltpu.make_async_remote_copy(
            src_ref=out.at[m], dst_ref=gin.at[m], send_sem=b_send.at[m], recv_sem=b_recv.at[m],
            device_id={"section": sec - 1}, device_id_type=MESH,
        )

    @pl.when(sec == 0)
    def _():
        hin[...] = entry[...]

    def live_keys(m):
        keys = lax.broadcasted_iota(jnp.int32, (GROUP_HEADS * length, length), 1)
        return keys < lengths[m]

    def attend(m):
        wide = hin[m].astype(F32)
        normed = (wide * rms_of(wide) * gain[...]).astype(BF16)
        x = rotate(dot_nn(normed, wqkv[...]), cos_ref[...], sin_ref[...]).astype(BF16)
        xs[m] = x
        keys = both_halves(x[:, qw : qw + 128])
        values = both_halves(x[:, qw + 128 : qw + 256])
        live = live_keys(m)
        stacks = []
        for group in range(KV_GROUPS):
            scores = dot_nt(stack_heads(x, group), keys[group]) * HEAD_DIM ** (-0.5)
            weights = jnp.where(live, jnp.exp(scores), 0.0)
            prob = weights / jnp.sum(weights, axis=-1, keepdims=True)
            probs[m, group] = prob
            stacks.append(dot_nn(prob.astype(BF16), values[group]))
        contexts[m] = merge_heads(stacks, length).astype(BF16)

    if ring:
        hop_send, hop_recv, side_send, side_recv, keep_sem = gathering[2:]
        chips = n_dp // 2
        reach = chips // 2
        core = lax.rem(rep, 2)
        chip = rep // 2

        def place(c):
            return c + (c // 2) * (1 - 2 * lax.rem(c, 2)) if chips == 4 else c

        at = place(chip)
        pieces = ((w_in, wqkv), (w_up, wout))

        def region(piece, shard, half):
            held = pieces[piece][1]
            rows = pieces[piece][0].shape[0]
            cols = held.shape[1]
            cut = (cols // 128 + 1) // 2 * 128
            span = {None: (0, cols), 0: (0, cut), 1: (cut, cols - cut)}[half]
            start = pl.multiple_of(shard * rows, rows)
            return held.at[pl.ds(start, rows), pl.ds(*span)]

        def own(piece, half):
            mine, held = pieces[piece]
            if half is None:
                return mine
            cols = held.shape[1]
            cut = (cols // 128 + 1) // 2 * 128
            return mine.at[:, pl.ds(*((0, cut), (cut, cols - cut))[half])]

        def half_of(way, step):
            return way if step == reach else None

        def hop(piece, way, step):
            turn = 1 if way == 0 else chips - 1
            source = place(lax.rem(at + (step - 1) * (chips - turn), chips)) * 2 + core
            half = half_of(way, step)
            target = place(lax.rem(at + turn, chips)) * 2 + core
            dst = region(piece, source, half)
            return pltpu.make_async_remote_copy(
                src_ref=own(piece, half) if step == 1 else dst, dst_ref=dst,
                send_sem=hop_send.at[piece, way, step - 1],
                recv_sem=hop_recv.at[piece, way, step - 1],
                device_id={"dp": target}, device_id_type=MESH,
            )

        def side(piece, way, step):
            turn = 1 if way == 0 else chips - 1
            source = place(lax.rem(at + step * (chips - turn), chips)) * 2 + core
            half = half_of(way, step)
            dst = region(piece, source, half)
            return pltpu.make_async_remote_copy(
                src_ref=own(piece, None) if step == 0 else dst, dst_ref=dst,
                send_sem=side_send.at[piece, way, step],
                recv_sem=side_recv.at[piece, way, step],
                device_id={"dp": chip * 2 + 1 - core}, device_id_type=MESH,
            )

        def keep(piece):
            return pltpu.make_async_copy(
                own(piece, None), region(piece, rep, None), keep_sem.at[piece]
            )

        sides = [(0, 0)] + [(way, step) for step in range(1, reach + 1) for way in (0, 1)]

        def begin(piece):
            for way in (0, 1):
                hop(piece, way, 1).start()
            side(piece, 0, 0).start()
            keep(piece).start()

        def advance(piece, step):
            for way in (0, 1):
                hop(piece, way, step).wait_recv()
                if step < reach:
                    hop(piece, way, step + 1).start()
                side(piece, way, step).start()

        def finish(piece):
            advance(piece, reach)
            keep(piece).wait()
            for way, step in sides:
                side(piece, way, step).wait_recv()

        begin(0)
        for step in range(1, reach):
            advance(0, step)
        begin(1)
        finish(0)

    def early(m, carry):
        if ring:
            @pl.when(m == seqs // 2)
            def _():
                for step in range(1, reach):
                    advance(1, step)

        @pl.when(sec == 0)
        def _():
            attend(m)

        return carry

    lax.fori_loop(0, seqs, early, 0)
    if ring:
        finish(1)

    def forward(m, carry):
        @pl.when(sec > 0)
        def _():
            forward_copy(m).wait_recv()
            attend(m)

        hout[m] = (hin[m].astype(F32) + dot_nn(contexts[m], wout[...])).astype(BF16)

        @pl.when(sec < last)
        def _():
            forward_copy(m).start()

        return carry

    lax.fori_loop(0, seqs, forward, 0)

    @pl.when(sec == last)
    def _():
        fgain = final_gain[...]
        row16 = lax.broadcasted_iota(jnp.int32, (16, part), 0)
        position = lax.broadcasted_iota(jnp.int32, (length, width), 0)
        own = jnp.zeros((16, part), F32)
        for j in range(seqs):
            picked = jnp.where(position == lengths[j] - 1, hout[j].astype(F32), 0.0)
            row = jnp.sum(picked, axis=0, keepdims=True)
            rows_buf[j] = row
            pooled = row * rms_of(row) * fgain
            unit = pooled * lax.rsqrt(jnp.sum(pooled * pooled, axis=-1, keepdims=True))
            for b in range(blocks):
                own = jnp.where(row16 == b * seqs + j, unit[:, b * part : (b + 1) * part], own)
        emb_all[rep] = own.astype(BF16)
        marks = jnp.zeros((8, 128), jnp.int32)
        mark_row = lax.broadcasted_iota(jnp.int32, (8, 128), 0)
        for i in range(micro):
            marks = jnp.where(mark_row == i, positive[i], marks)
        pos_all[rep] = marks

        def exchange(step):
            to = peer(step)
            return [
                pltpu.make_async_remote_copy(
                    src_ref=buf.at[rep], dst_ref=buf.at[rep],
                    send_sem=send.at[step], recv_sem=recv.at[step],
                    device_id={"dp": to}, device_id_type=MESH,
                )
                for buf, send, recv in ((emb_all, e_send, e_recv), (pos_all, p_send, p_recv))
            ]

        copies = [exchange(step) for step in range(1, n_dp)]
        for pair in copies:
            for copy in pair:
                copy.start()
        for pair in copies:
            for copy in pair:
                copy.wait()

        total = n_dp * seqs
        tall = n_dp * 16
        everyone = emb_all[...].reshape(tall, part)
        cross = dot_nt(everyone, everyone)
        ra = lax.broadcasted_iota(jnp.int32, (tall, tall), 0)
        ca = lax.broadcasted_iota(jnp.int32, (tall, tall), 1)
        same = lax.rem(ra, 16) // seqs == lax.rem(ca, 16) // seqs
        cross = jnp.where(same, cross, 0.0)
        fr = lax.broadcasted_iota(jnp.int32, (total, tall), 0)
        fc = lax.broadcasted_iota(jnp.int32, (total, tall), 1)
        fold = (fc // 16 * seqs + lax.rem(fc, seqs) == fr).astype(F32)
        logits = SHARPNESS * lax.dot_general(
            dot_hi(fold, cross), fold, (((1,), (1,)), ((), ())),
            preferred_element_type=F32, precision=HI,
        )
        qr = lax.broadcasted_iota(jnp.int32, (total, total), 0)
        dc = lax.broadcasted_iota(jnp.int32, (total, total), 1)
        doc = lax.rem(dc, 2) == 1
        weights = jnp.where(doc, jnp.exp(logits), 0.0)
        odds = weights / jnp.sum(weights, axis=-1, keepdims=True)
        marks_all = pos_all[...].reshape(n_dp * 8, 128).astype(F32)
        pr = lax.broadcasted_iota(jnp.int32, (total, n_dp * 8), 0)
        pc = lax.broadcasted_iota(jnp.int32, (total, n_dp * 8), 1)
        pick = (pr // seqs * 8 + lax.rem(pr, seqs) // 2 == pc).astype(F32)
        target = dot_hi(pick, marks_all)[:, :1]
        hit = jnp.logical_and(doc, (dc // 2).astype(F32) == target).astype(F32)
        coef = (odds - hit) * (COEF * SHARPNESS)
        coef = jnp.where(lax.rem(qr, 2) == 0, coef, 0.0)
        both = coef + coef.T
        ar = lax.broadcasted_iota(jnp.int32, (16, total), 0)
        ac = lax.broadcasted_iota(jnp.int32, (16, total), 1)
        mine = (rep * seqs + lax.rem(ar, seqs) == ac).astype(F32)
        spread = dot_hi(dot_hi(mine, both), fold)
        br = lax.broadcasted_iota(jnp.int32, (16, tall), 0)
        bc = lax.broadcasted_iota(jnp.int32, (16, tall), 1)
        spread = jnp.where(br // seqs == lax.rem(bc, 16) // seqs, spread, 0.0)
        grad16 = dot_hi(spread, everyone.astype(F32))
        for j in range(seqs):
            grad_e = jnp.concatenate(
                [grad16[b * seqs + j : b * seqs + j + 1] for b in range(blocks)], axis=1
            )
            row = rows_buf[j]
            scale = rms_of(row)
            pooled = row * scale * fgain
            size = lax.rsqrt(jnp.sum(pooled * pooled, axis=-1, keepdims=True))
            unit = pooled * size
            grad_f = size * (grad_e - unit * jnp.sum(unit * grad_e, axis=-1, keepdims=True))
            grad_n = grad_f * fgain
            grad_r = grad_n * scale - row * (
                scale * scale * scale * jnp.mean(row * grad_n, axis=-1, keepdims=True)
            )
            gin[j] = jnp.where(position == lengths[j] - 1, grad_r, 0.0).astype(BF16)

    def backward(m, carry):
        @pl.when(sec < last)
        def _():
            backward_copy(m).wait_recv()

        grad = gin[m]
        x = xs[m]
        keys = both_halves(x[:, qw : qw + 128])
        values = both_halves(x[:, qw + 128 : qw + 256])
        grad_ctx = dot_nt(grad, wout[...]).astype(BF16)
        grad_q, grad_k, grad_v = [], [], []
        for group in range(KV_GROUPS):
            prob = probs[m, group]
            upper = stack_heads(grad_ctx, group)
            grad_p = dot_nt(upper, values[group]).astype(BF16).astype(F32)
            grad_v.append(dot_tn(prob.astype(BF16), upper))
            inner = jnp.sum(grad_p * prob, axis=-1, keepdims=True)
            grad_s = (prob * (grad_p - inner) * HEAD_DIM ** (-0.5)).astype(BF16)
            grad_q.append(dot_nn(grad_s, keys[group]))
            grad_k.append(dot_tn(grad_s, stack_heads(x, group)))
        grad_x = jnp.concatenate(
            [merge_heads(grad_q, length), fold_groups(grad_k), fold_groups(grad_v)], axis=1
        )
        grad_x = grad_x.astype(BF16).astype(F32)
        grad_x = rotate(grad_x, cos_ref[...], -sin_ref[...]).astype(BF16)
        grad_n = dot_nt(grad_x, wqkv[...]).astype(BF16).astype(F32) * gain[...]
        wide = hin[m].astype(F32)
        scale = rms_of(wide)
        slope = scale * scale * scale * jnp.mean(wide * grad_n, axis=-1, keepdims=True)
        out[m] = (grad.astype(F32) + grad_n * scale - wide * slope).astype(BF16)

        @pl.when(sec > 0)
        def _():
            backward_copy(m).start()

        return carry

    lax.fori_loop(0, seqs, backward, 0)

    @pl.when(sec < last)
    def _():
        for m in range(seqs):
            forward_copy(m).wait_send()

    @pl.when(sec > 0)
    def _():
        for m in range(seqs):
            backward_copy(m).wait_send()

    if ring:
        for piece in (0, 1):
            for way in (0, 1):
                for step in range(1, reach + 1):
                    hop(piece, way, step).wait_send()
            for way, step in sides:
                side(piece, way, step).wait_send()


def tables(length, qw, columns):
    lane = np.arange(columns)
    half = HEAD_DIM // 2
    frequency = np.float32(ROPE_BASE) ** (
        -(lane % half).astype(np.float32) * np.float32(2.0 / HEAD_DIM)
    )
    angles = np.arange(length, dtype=np.float32)[:, None] * frequency[None, :]
    turned = (lane < columns - KV_GROUPS * HEAD_DIM)[None, :]
    sign = np.where(lane % HEAD_DIM < half, -1.0, 1.0)[None, :]
    cos = np.where(turned, np.cos(angles), 1.0).astype(np.float32)
    sin = np.where(turned, np.sin(angles) * sign, 0.0).astype(np.float32)
    return jnp.asarray(cos), jnp.asarray(sin)


def per_device(entry, norm_gain, w_qkv, w_out, final_gain, lengths, positive):
    n_sec = lax.axis_size("section")
    n_dp = lax.axis_size("dp")
    seqs = lengths.shape[0]
    rows, width = entry.shape
    length = rows // seqs
    qw = w_out.shape[1] * n_dp
    columns = w_qkv.shape[2]
    ring = w_qkv.shape[1] % 16 == 0 and w_out.shape[1] % 16 == 0 and n_dp % 4 == 0
    if ring:
        full_qkv, full_out = w_qkv[0], w_out[0]
    else:
        full_qkv = lax.all_gather(w_qkv, "dp", axis=1, tiled=True)[0]
        full_out = lax.all_gather(w_out, "dp", axis=1, tiled=True)[0]
    reach = n_dp // 4
    gathering = [
        pltpu.VMEM((width, columns), BF16),
        pltpu.VMEM((qw, width), BF16),
        pltpu.SemaphoreType.DMA((2, 2, reach)),
        pltpu.SemaphoreType.DMA((2, 2, reach)),
        pltpu.SemaphoreType.DMA((2, 2, reach + 1)),
        pltpu.SemaphoreType.DMA((2, 2, reach + 1)),
        pltpu.SemaphoreType.DMA((2,)),
    ] if ring else []
    cos, sin = tables(length, qw, columns)
    vmem = pl.BlockSpec(memory_space=pltpu.VMEM)
    smem = pl.BlockSpec(memory_space=pltpu.SMEM)
    part = width // (16 // seqs)
    dma = pltpu.SemaphoreType.DMA
    block = (seqs, length, width)
    result = pl.pallas_call(
        functools.partial(kernel, n_sec, n_dp, seqs, length, ring),
        out_shape=jax.ShapeDtypeStruct(block, BF16),
        in_specs=[vmem] * 7 + [smem] * 2,
        out_specs=vmem,
        scratch_shapes=[
            pltpu.VMEM(block, BF16),
            pltpu.VMEM(block, BF16),
            pltpu.VMEM(block, BF16),
            pltpu.VMEM((seqs, length, columns), BF16),
            pltpu.VMEM((seqs, KV_GROUPS, GROUP_HEADS * length, length), F32),
            pltpu.VMEM((seqs, 1, width), F32),
            pltpu.VMEM((n_dp, 16, part), BF16),
            pltpu.VMEM((n_dp, 8, 128), jnp.int32),
            pltpu.VMEM((seqs, length, qw), BF16),
            dma((seqs,)), dma((seqs,)), dma((seqs,)), dma((seqs,)),
            dma((n_dp,)), dma((n_dp,)), dma((n_dp,)), dma((n_dp,)),
            *gathering,
        ],
        compiler_params=pltpu.CompilerParams(
            collective_id=0, has_side_effects=True, vmem_limit_bytes=60 * 1024 * 1024
        ),
    )(
        entry.reshape(block), norm_gain, full_qkv, full_out, final_gain.reshape(1, width),
        cos, sin, lengths, positive,
    )
    return result.reshape(1, rows, width)


def solution(mesh):
    return jax.shard_map(
        per_device,
        mesh=mesh,
        in_specs=(
            P("dp", None),
            P("section", None),
            P("section", "dp", None),
            P("section", "dp", None),
            P(),
            P("dp"),
            P("dp"),
        ),
        out_specs=P("section", "dp", None),
        check_vma=False,
    )
```
